32 devices in a mesh: member: 8 (over z, core), space: 4 (over y, x).
Axes of the slice: x: 2, y: 2, z: 4, core: 2. Of those that a mesh axis runs over, the one named last changes fastest.
Arguments:
- weather: bfloat16 [8, 84, 64, 1440], P('member', None, 'space'), may hold values from -6 to 6
- coefficients: int32 [8, 84, 2, 364, 361], P('member', None, None, 'space'), may hold values from -1073741824 to 1073741823
- channel_scale: float32 [84], replicated, may hold values from 0.3 to 3
Outputs:
- perturbed: bfloat16 [8, 84, 64, 1440], P('member', None, 'space')
The draws below stay inside these ranges and needn't reach their ends.
All inputs are finite; a program needn't handle non-finite values.
Results may differ from the reference program's by a relative error of at most 0.007.
Values may be sent and summed in bfloat16 or wider, within the bound.
A program may use at most 192 MiB of HBM per device.

```python
import math
import jax
import jax.numpy as jnp
from jax import lax

CH = 84
LON = 1440
E = 8
LAT = 64
LAT0 = 328
LP = 361
MP = 364


def with_ends(values, rng, low, largest):
    longest = values.shape.index(max(values.shape))
    spots = []
    for shift in (0, 1):
        where = [jax.random.randint(jax.random.fold_in(rng, axis), (), 0, length) for axis, length in enumerate(values.shape)]
        where[longest] = (where[longest] + shift) % values.shape[longest]
        spots.append(tuple(where))
    return values.at[spots[0]].set(low).at[spots[1]].set(largest)


def shard_levels(key, extent, pieces, least, high):
    level = 1.0
    for position, blocks in pieces:
        heights = jax.random.uniform(jax.random.fold_in(jax.random.fold_in(key, 6), position), (blocks,), jnp.float32, least / len(pieces), high / len(pieces))
        level = level * jnp.repeat(jnp.exp(heights), extent[position] // blocks).reshape((-1,) + (1,) * (len(extent) - 1 - position))
    return level


def normal_values(own_key, dims, spread, reach, shards=(), kind=jnp.bfloat16):
    loudness = shard_levels(own_key, dims, shards, -0.22, 0.18) if shards else 1.0
    values = jax.random.normal(own_key, dims, jnp.float32) * spread * loudness
    return jnp.minimum(jnp.maximum(values, -reach), reach).astype(kind)


def setup_inputs(seed: int = 0) -> dict:
    key_list = jax.random.split(jax.random.key(seed), 4)
    weather = normal_values(key_list[0], (E, CH, LAT, LON), 1.0, 6.0, ((0, 8), (2, 4)))
    coefficients = with_ends(jax.random.randint(key_list[1], (E, CH, 2, MP, LP), -1073741824, 1073741824), jax.random.fold_in(key_list[1], 1), -1073741824, 1073741823).astype(jnp.int32)
    channel_scale = jnp.clip(jnp.exp(jax.random.uniform(key_list[2], (CH,), jnp.float32, math.log(0.3), math.log(3.0))), 0.3, 3.0)
    return dict(weather=weather, coefficients=coefficients, channel_scale=channel_scale)


def diagonal_log(order_count):
    steps_up = jnp.arange(1, order_count, dtype=jnp.int32).astype(jnp.float32)
    terms = 0.5 * jnp.log((2.0 * steps_up + 1.0) / (2.0 * steps_up))
    return jnp.concatenate([jnp.zeros((1,), jnp.float32), jnp.cumsum(terms)])

def legendre_table(orders, colatitude, order_logs, degree_count):
    order_values = orders.astype(jnp.float32)[:, None]
    cosine = jnp.cos(colatitude)[None, :]
    sine_values = jnp.sin(colatitude)[None, :]
    diagonal = jnp.exp(order_logs[:, None] - 0.5 * math.log(4.0 * math.pi) + order_values * jnp.log(sine_values))
    block_size = 16
    turn_count = (degree_count + block_size - 1) // block_size
    order_square = order_values * order_values

    def advance(carry, turn_index):
        older_row, newer_row = carry
        produced = []
        for inner_step in range(block_size):
            degree = (turn_index * block_size + inner_step).astype(jnp.float32)
            degree_square = degree * degree
            prior = degree - 1.0
            factor_up = jnp.sqrt(jnp.maximum(4.0 * degree_square - 1.0, 1.0) / jnp.maximum(degree_square - order_square, 1.0))
            factor_down = jnp.sqrt(jnp.maximum(prior * prior - order_square, 0.0) / jnp.maximum(4.0 * prior * prior - 1.0, 1.0))
            next_row = factor_up * (cosine * newer_row - factor_down * older_row)
            next_row = jnp.where(degree < order_values, 0.0, jnp.where(degree == order_values, diagonal, next_row))
            produced.append(next_row)
            older_row, newer_row = (newer_row, next_row)
        return ((older_row, newer_row), jnp.stack(produced))
    empty = jnp.zeros_like(diagonal)
    carried, stacked = lax.scan(advance, (empty, empty), jnp.arange(turn_count, dtype=jnp.int32))
    return stacked.reshape(turn_count * block_size, orders.shape[0], colatitude.shape[0])[:degree_count]

def spectral_values(coefficients, orders):
    degree_count = coefficients.shape[-1]
    degrees = jnp.arange(degree_count, dtype=jnp.int32)
    keep = degrees[None, :] >= orders[:, None]
    factor = math.sqrt(3.0) * math.sqrt(4.0 * math.pi) / degree_count * 2.0 ** (-30)
    values = coefficients.astype(jnp.float32) * factor
    return jnp.where(keep, values, 0.0).astype(jnp.bfloat16)

def fourier_basis(order_count, lon_count):
    orders = jnp.arange(order_count, dtype=jnp.int32)
    columns = jnp.arange(lon_count, dtype=jnp.int32)
    phases = orders[:, None] * columns[None, :] % lon_count
    angles = 2.0 * math.pi / lon_count * phases.astype(jnp.float32)
    weights = jnp.where(orders == 0, 1.0, math.sqrt(2.0)).astype(jnp.float32)[:, None]
    return jnp.stack([weights * jnp.cos(angles), weights * jnp.sin(angles)]).astype(jnp.bfloat16)

def reference(weather, coefficients, channel_scale):
    orders = jnp.arange(MP, dtype=jnp.int32)
    colatitude = math.pi * (LAT0 + jnp.arange(LAT, dtype=jnp.int32)).astype(jnp.float32) / (LON // 2)
    legendre = legendre_table(orders, colatitude, diagonal_log(MP), LP).astype(jnp.bfloat16)
    legendre_wide = lax.optimization_barrier(legendre).astype(jnp.float32)
    basis = fourier_basis(MP, LON).reshape(2 * MP, LON)

    def one_member(coef_member):
        spectral = lax.optimization_barrier(spectral_values(coef_member, orders)).astype(jnp.float32)
        fourier = jnp.einsum('cpml,lmt->ctpm', spectral, legendre_wide, precision=lax.Precision.HIGHEST).astype(jnp.bfloat16)
        noise = jnp.dot(fourier.reshape(CH * LAT, 2 * MP), basis, preferred_element_type=jnp.float32)
        return noise.astype(jnp.bfloat16).reshape(CH, LAT, LON)
    noise_all = lax.map(one_member, coefficients)

    def add_up(total, noise_member):
        return (total + noise_member.astype(jnp.float32), None)
    total, unused = lax.scan(add_up, jnp.zeros((CH, LAT, LON), jnp.float32), noise_all)
    mean = total / E

    def perturb(pair):
        weather_member, noise_member = pair
        centred = noise_member.astype(jnp.float32) - mean
        return (weather_member.astype(jnp.float32) + channel_scale[:, None, None] * centred).astype(jnp.bfloat16)
    return lax.map(perturb, (weather, noise_all))
```

```python
import functools
import math

import jax
import jax.numpy as jnp
from jax import lax
from jax.experimental import pallas as pl
from jax.experimental.pallas import tpu as pltpu
from jax.sharding import PartitionSpec as P


def round_up(value, step):
    return (value + step - 1) // step * step


def diagonal_log(order_count):
    steps_up = jnp.arange(1, order_count, dtype=jnp.int32).astype(jnp.float32)
    terms = 0.5 * jnp.log((2.0 * steps_up + 1.0) / (2.0 * steps_up))
    return jnp.concatenate([jnp.zeros((1,), jnp.float32), jnp.cumsum(terms)])


def synthesis_kernel(block, pitch, order_ref, cosine_ref, diagonal_ref, spectral_ref, out_ref, table):
    half, lanes = order_ref.shape
    degrees = spectral_ref.shape[-1]

    @pl.when(pl.program_id(0) == 0)
    def build():
        order = order_ref[...]
        order_square = order * order
        cosine = jnp.broadcast_to(cosine_ref[...], (half, lanes))
        diagonal = diagonal_ref[...]

        def advance(step, carry):
            older, newer, down = carry
            degree = step.astype(jnp.float32)
            wide = jnp.full((half, lanes), degree, jnp.float32)
            square = wide * wide
            ratio = jnp.maximum(square - order_square, 0.25) / jnp.maximum(4.0 * square - 1.0, 1.0)
            up = lax.rsqrt(ratio)
            row = up * (cosine * newer - down * older)
            row = jnp.where(wide < order, 0.0, jnp.where(wide == order, diagonal, row))
            for tile in range(lanes // 128):
                table[pl.ds(tile * half * pitch + step, half, stride=pitch), :] = row[
                    :, tile * 128 : tile * 128 + 128
                ]
            return newer, row, ratio * up

        zero = order * 0.0
        lax.fori_loop(0, degrees, advance, (zero, zero, zero), unroll=4)

    first = pl.program_id(0) * block
    rows = spectral_ref.shape[2]
    low = lax.broadcasted_iota(jnp.int32, (rows, lanes), 1) < lanes // 2
    for inner in range(block):
        tiles = []
        for tile in range(lanes // 128):
            start = pl.multiple_of((tile * half + first + inner) * pitch, 8)
            tiles.append(table[pl.ds(start, degrees), :].astype(jnp.bfloat16))
        values = jnp.concatenate(tiles, axis=1)
        both = jnp.concatenate([spectral_ref[0, inner], spectral_ref[1, inner]], axis=0)
        found = jnp.dot(both, values, preferred_element_type=jnp.float32)
        out_ref[inner] = jnp.where(low, found[:rows], found[rows:]).astype(jnp.bfloat16)


def synthesize(spectral, order_plane, cosine_row, diagonal_plane):
    pair, half, rows, degrees = spectral.shape
    lanes = order_plane.shape[1]
    block = 8
    pitch = degrees + 8
    return pl.pallas_call(
        functools.partial(synthesis_kernel, block, pitch),
        grid=(half // block,),
        out_shape=jax.ShapeDtypeStruct((half, rows, lanes), jnp.bfloat16),
        in_specs=[
            pl.BlockSpec((half, lanes), lambda i: (0, 0)),
            pl.BlockSpec((1, lanes), lambda i: (0, 0)),
            pl.BlockSpec((half, lanes), lambda i: (0, 0)),
            pl.BlockSpec((pair, block, rows, degrees), lambda i: (0, i, 0, 0)),
        ],
        out_specs=pl.BlockSpec((block, rows, lanes), lambda i: (i, 0, 0)),
        scratch_shapes=[pltpu.VMEM((lanes // 128 * half * pitch, 128), jnp.float32)],
        compiler_params=pltpu.CompilerParams(vmem_limit_bytes=60 * 1024 * 1024),
    )(order_plane, cosine_row, diagonal_plane, spectral)


def local(weather, coefficients, channel_scale):
    group_count = lax.axis_size("member")
    band_count = lax.axis_size("space")
    member_local, channels, rows_local, lon_count = weather.shape
    order_local = coefficients.shape[3]
    degree_count = coefficients.shape[4]
    order_count = order_local * band_count
    lat_count = rows_local * band_count
    member_count = member_local * group_count
    rows = member_local * channels * 2
    half = round_up(order_local, 16) // 2
    padded = 2 * half
    degrees_padded = round_up(degree_count, 128)

    first_order = lax.axis_index("space") * order_local
    slots = jnp.arange(padded, dtype=jnp.int32)
    orders = first_order + slots
    logs = jnp.pad(diagonal_log(order_count), (0, padded))
    order_logs = lax.dynamic_slice_in_dim(logs, first_order, padded)
    row_first = (lon_count // 2 + 1 - lat_count) // 2
    colatitude = (
        math.pi
        * (row_first + jnp.arange(lat_count, dtype=jnp.int32)).astype(jnp.float32)
        / (lon_count // 2)
    )
    order_values = orders.astype(jnp.float32)[:, None]
    diagonal = jnp.exp(
        order_logs[:, None]
        - 0.5 * math.log(4.0 * math.pi)
        + order_values * jnp.log(jnp.sin(colatitude))[None, :]
    )

    def pair_up(plane):
        return jnp.concatenate([plane[:half], plane[half:]], axis=1)

    order_plane = pair_up(jnp.broadcast_to(order_values, (padded, lat_count)))
    cosine_row = jnp.tile(jnp.cos(colatitude), 2)[None, :]

    degrees = jnp.arange(degree_count, dtype=jnp.int32)
    keep = degrees[None, :] >= orders[:order_local, None]
    factor = math.sqrt(3.0) * math.sqrt(4.0 * math.pi) / degree_count * 2.0 ** (-30)
    spectral = jnp.where(keep, coefficients.astype(jnp.float32) * factor, 0.0).astype(jnp.bfloat16)
    spectral = spectral.transpose(3, 0, 1, 2, 4).reshape(order_local, rows, degree_count)
    spectral = jnp.pad(
        spectral, ((0, padded - order_local), (0, 0), (0, degrees_padded - degree_count))
    ).reshape(2, half, rows, degrees_padded)
    found = synthesize(spectral, order_plane, cosine_row, pair_up(diagonal))

    found = found.reshape(half, member_local * channels, 2, 2, band_count, rows_local)
    found = found.transpose(4, 3, 2, 0, 1, 5)
    depth = padded * 2
    flat = member_local * channels * rows_local
    found = found.reshape(band_count, depth, flat)
    own = lax.all_to_all(found, "space", split_axis=0, concat_axis=0, tiled=True)

    band = jnp.arange(band_count, dtype=jnp.int32)[:, None]
    slot = slots.reshape(2, half)
    row_order = band * order_local + slots[None, :]
    real_slot = jnp.broadcast_to(slots[None, :] < order_local, row_order.shape)
    columns = jnp.arange(lon_count, dtype=jnp.int32)
    phases = row_order[:, :, None] * columns % lon_count
    angles = 2.0 * math.pi / lon_count * phases.astype(jnp.float32)
    weights = jnp.where(real_slot, jnp.where(row_order == 0, 1.0, math.sqrt(2.0)), 0.0)
    weights = weights.astype(jnp.float32)[:, :, None]
    shape = (band_count, 2, half, lon_count)
    basis = jnp.stack(
        [(weights * jnp.cos(angles)).reshape(shape), (weights * jnp.sin(angles)).reshape(shape)], axis=2
    ).astype(jnp.bfloat16)
    basis = basis.reshape(band_count * depth, lon_count)

    own = own.reshape(band_count * depth, flat)
    split = own.astype(jnp.float32).reshape(band_count * depth, member_local, -1)
    total = lax.psum(jnp.sum(split, axis=1).astype(jnp.bfloat16), "member").astype(jnp.float32)
    centred = (split - total[:, None, :] * (1.0 / member_count)).astype(jnp.bfloat16)
    centred = centred.reshape(band_count * depth, flat)
    noise = lax.dot_general(
        centred, basis, (((0,), (0,)), ((), ())), preferred_element_type=jnp.float32
    )
    noise = noise.reshape(member_local, channels, rows_local, lon_count)
    scale_wide = channel_scale[None, :, None, None]
    return (weather.astype(jnp.float32) + scale_wide * noise).astype(jnp.bfloat16)


def solution(mesh):
    return jax.shard_map(
        local,
        mesh=mesh,
        in_specs=(P("member", None, "space", None), P("member", None, None, "space", None), P()),
        out_specs=P("member", None, "space", None),
        check_vma=False,
    )
```

```python
import functools
import math

import jax
import jax.numpy as jnp
from jax import lax
from jax.experimental import pallas as pl
from jax.experimental.pallas import tpu as pltpu
from jax.sharding import PartitionSpec as P


def round_up(value, step):
    return (value + step - 1) // step * step


def diagonal_log(order_count):
    steps_up = jnp.arange(1, order_count, dtype=jnp.int32).astype(jnp.float32)
    terms = 0.5 * jnp.log((2.0 * steps_up + 1.0) / (2.0 * steps_up))
    return jnp.concatenate([jnp.zeros((1,), jnp.float32), jnp.cumsum(terms)])


def spectral_kernel(order_local, degree_count, pitch, coef_ref, out_ref, turned):
    rows, padded, degrees = coef_ref.shape
    first = lax.axis_index("space") * order_local
    factor = math.sqrt(3.0) * math.sqrt(4.0 * math.pi) / degree_count * 2.0 ** (-30)
    tiles = degrees // 128
    keeps = []
    for tile in range(tiles):
        slot = lax.broadcasted_iota(jnp.int32, (padded, 128), 0)
        degree = lax.broadcasted_iota(jnp.int32, (padded, 128), 1) + tile * 128
        keeps.append((degree >= slot + first) & (degree < degree_count) & (slot < order_local))

    def convert(row, carry):
        for tile in range(tiles):
            values = coef_ref[row, :, tile * 128 : tile * 128 + 128].astype(jnp.float32) * factor
            start = pl.multiple_of((tile * rows + row) * pitch, 8)
            turned[pl.ds(start, padded), :] = jnp.where(keeps[tile], values, 0.0)
        return carry

    lax.fori_loop(0, rows, convert, 0)

    def collect(slot, carry):
        for tile in range(tiles):
            values = turned[pl.ds(tile * rows * pitch + slot, rows, stride=pitch), :]
            out_ref[slot, :, tile * 128 : tile * 128 + 128] = values.astype(jnp.bfloat16)
        return carry

    lax.fori_loop(0, padded, collect, 0, unroll=8)


def turn_spectral(coefficients, padded, degrees, degree_count):
    rows, order_local, _ = coefficients.shape
    block = 24 if rows % 24 == 0 else 8
    pitch = padded + 8
    return pl.pallas_call(
        functools.partial(spectral_kernel, order_local, degree_count, pitch),
        grid=(rows // block,),
        out_shape=jax.ShapeDtypeStruct((padded, rows, degrees), jnp.bfloat16),
        in_specs=[pl.BlockSpec((block, padded, degrees), lambda i: (i, 0, 0))],
        out_specs=pl.BlockSpec((padded, block, degrees), lambda i: (0, i, 0)),
        scratch_shapes=[pltpu.VMEM((degrees // 128 * block * pitch, 128), jnp.float32)],
        compiler_params=pltpu.CompilerParams(vmem_limit_bytes=48 * 1024 * 1024),
    )(coefficients)


def synthesis_kernel(
    block, pitch, lat, order_ref, cosine_ref, diagonal_ref, spectral_ref, out_ref, table, kept
):
    half, lanes = order_ref.shape
    degrees = spectral_ref.shape[-1]

    @pl.when(pl.program_id(0) == 0)
    def build():
        order = order_ref[...]
        order_square = order * order
        cosine = jnp.broadcast_to(cosine_ref[...], (half, lanes))
        diagonal = diagonal_ref[...]

        def advance(step, carry):
            older, newer, down = carry
            degree = step.astype(jnp.float32)
            wide = jnp.full((half, lanes), degree, jnp.float32)
            square = wide * wide
            ratio = jnp.maximum(square - order_square, 0.25) / jnp.maximum(4.0 * square - 1.0, 1.0)
            up = lax.rsqrt(ratio)
            row = up * (cosine * newer - down * older)
            row = jnp.where(wide < order, 0.0, jnp.where(wide == order, diagonal, row))
            for tile in range(lanes // 128):
                table[pl.ds(tile * half * pitch + step, half, stride=pitch), :] = row[
                    :, tile * 128 : tile * 128 + 128
                ]
            return newer, row, ratio * up

        zero = order * 0.0
        lax.fori_loop(0, degrees, advance, (zero, zero, zero), unroll=4)

    first = pl.program_id(0) * block
    rows = spectral_ref.shape[2]
    low = lax.broadcasted_iota(jnp.int32, (rows, lanes), 1) < lanes // 2
    pack = 128 // lat
    bands = lanes // 2 // lat
    groups = out_ref.shape[-1] // 128
    kept_rows = groups * pack * 2
    deep = half + 8
    for inner in range(block):
        tiles = []
        for tile in range(lanes // 128):
            start = pl.multiple_of((tile * half + first + inner) * pitch, 8)
            tiles.append(table[pl.ds(start, degrees), :].astype(jnp.bfloat16))
        values = jnp.concatenate(tiles, axis=1)
        both = jnp.concatenate([spectral_ref[0, inner], spectral_ref[1, inner]], axis=0)
        found = jnp.dot(both, values, preferred_element_type=jnp.float32)
        found = jnp.where(low, found[:rows], found[rows:])
        for tile in range(lanes // 128):
            kept[pl.ds(tile * kept_rows * deep + first + inner, rows, stride=deep), :] = found[
                :, tile * 128 : tile * 128 + 128
            ]

    @pl.when(pl.program_id(0) == pl.num_programs(0) - 1)
    def regroup():
        chunk = lax.broadcasted_iota(jnp.int32, (half, 128), 1) // lat
        for tile in range(lanes // 128):
            for spare in range(rows, kept_rows):
                kept[pl.ds((tile * kept_rows + spare) * deep, half), :] = order_ref[:, :128] * 0.0

            def one_group(group, carry):
                for part in range(2):
                    planes = []
                    for spot in range(pack):
                        row = tile * kept_rows + (group * pack + spot) * 2 + part
                        planes.append(kept[pl.ds(pl.multiple_of(row * deep, 8), half), :])
                    gap = 1
                    while gap < pack:
                        upper = (chunk // gap) % 2 == 1
                        for spot in range(pack):
                            if (spot // gap) % 2 == 0:
                                one, two = planes[spot], planes[spot + gap]
                                planes[spot] = jnp.where(upper, pltpu.roll(two, gap * lat, 1), one)
                                planes[spot + gap] = jnp.where(
                                    upper, two, pltpu.roll(one, 128 - gap * lat, 1)
                                )
                        gap *= 2
                    for spot in range(pack):
                        high, band = divmod(tile * pack + spot, bands)
                        lane = pl.multiple_of(group * 128, 128)
                        out_ref[band, high, part, :, pl.ds(lane, 128)] = planes[spot].astype(
                            jnp.bfloat16
                        )
                return carry

            lax.fori_loop(0, groups, one_group, 0)


def synthesize(spectral, order_plane, cosine_row, diagonal_plane, lat):
    pair, half, rows, degrees = spectral.shape
    lanes = order_plane.shape[1]
    block = 8
    pitch = degrees + 8
    pack = 128 // lat
    groups = round_up(rows // 2, pack) // pack
    out_dims = (lanes // 2 // lat, 2, 2, half, groups * 128)
    kept_rows = lanes // 128 * groups * pack * 2 * (half + 8)
    return pl.pallas_call(
        functools.partial(synthesis_kernel, block, pitch, lat),
        grid=(half // block,),
        out_shape=jax.ShapeDtypeStruct(out_dims, jnp.bfloat16),
        in_specs=[
            pl.BlockSpec((half, lanes), lambda i: (0, 0)),
            pl.BlockSpec((1, lanes), lambda i: (0, 0)),
            pl.BlockSpec((half, lanes), lambda i: (0, 0)),
            pl.BlockSpec((pair, block, rows, degrees), lambda i: (0, i, 0, 0)),
        ],
        out_specs=pl.BlockSpec(out_dims, lambda i: (0, 0, 0, 0, 0)),
        scratch_shapes=[
            pltpu.VMEM((lanes // 128 * half * pitch, 128), jnp.float32),
            pltpu.VMEM((kept_rows, 128), jnp.float32),
        ],
        compiler_params=pltpu.CompilerParams(vmem_limit_bytes=60 * 1024 * 1024),
    )(order_plane, cosine_row, diagonal_plane, spectral)


def exchange_kernel(parts, sent, out, raw, near, sums, lower, other, total, *sems):
    a2a_send, a2a_recv = sems[0], sems[1]
    pair = {
        "near": (sems[2], sems[3]),
        "line": (sems[4], sems[5]),
        "swap": (sems[6], sems[7]),
        "back": (sems[8], sems[9]),
        "mate": (sems[10], sems[11]),
    }
    bands, depth, _ = sent.shape
    member_count = lax.axis_size("member")
    chips = member_count // 2
    middle = chips // 2
    me = lax.axis_index("member")
    space = lax.axis_index("space")
    core = lax.rem(me, 2)
    chip = me // 2
    mate = chip * 2 + 1 - core
    left = chip < middle
    rank = jnp.where(left, chip, chips - 1 - chip)
    inward = jnp.where(left, chip + 1, chip - 1) * 2 + core
    outward = jnp.where(left, chip - 1, chip + 1) * 2 + core
    step = depth // (2 * parts)
    mesh_ids = pl.DeviceIdType.MESH

    def spread(k, hop):
        rows = pl.ds(k * 2 * step, 2 * step)
        target = lax.rem(space + hop, bands)
        return pltpu.make_async_remote_copy(
            src_ref=sent.at[target, rows],
            dst_ref=raw.at[space, rows],
            send_sem=a2a_send.at[k, hop],
            recv_sem=a2a_recv.at[k, hop],
            device_id={"space": target},
            device_id_type=mesh_ids,
        )

    def hand(kind, k, source, landing, target):
        return pltpu.make_async_remote_copy(
            src_ref=source,
            dst_ref=landing,
            send_sem=pair[kind][0].at[k],
            recv_sem=pair[kind][1].at[k],
            device_id={"member": target},
            device_id_type=mesh_ids,
        )

    def half_rows(k, which):
        return pl.ds(pl.multiple_of((k * 2 + which) * step, step), step)

    def near_copy(k):
        return hand("near", k, raw.at[:, half_rows(k, 1 - core)], near.at[k], mate)

    def line_copy(k):
        return hand("line", k, sums.at[k], lower.at[k], inward)

    def swap_copy(k):
        return hand("swap", k, sums.at[k], other.at[k], inward)

    def back_copy(k):
        return hand("back", k, total.at[k, core], total.at[k, core], outward)

    def mate_copy(k):
        return hand("mate", k, total.at[k, core], total.at[k, core], mate)

    def stage_near(k):
        for hop in range(1, bands):
            spread(k, hop).wait_recv()
        near_copy(k).start()

    def send_inward(k, level):
        @pl.when(rank == level)
        def _():
            if level == middle - 1:
                swap_copy(k).start()
            else:
                line_copy(k).start()

    def stage_sum(k):
        near_copy(k).wait_recv()
        mine = raw[:, half_rows(k, core)].astype(jnp.float32) + near[k].astype(jnp.float32)
        sums[k] = mine.astype(jnp.bfloat16)
        send_inward(k, 0)

    def stage_line(level, k):
        @pl.when(rank == level)
        def _():
            line_copy(k).wait_recv()
            both = sums[k].astype(jnp.float32) + lower[k].astype(jnp.float32)
            sums[k] = both.astype(jnp.bfloat16)

        send_inward(k, level)

    def send_outward(k, level):
        if level > 0:
            back_copy(k).start()
        mate_copy(k).start()

    def stage_swap(k):
        @pl.when(rank == middle - 1)
        def _():
            swap_copy(k).wait_recv()
            both = sums[k].astype(jnp.float32) + other[k].astype(jnp.float32)
            total[k, core] = both.astype(jnp.bfloat16)
            send_outward(k, middle - 1)

    def stage_back(level, k):
        @pl.when(rank == level)
        def _():
            back_copy(k).wait_recv()
            send_outward(k, level)

    def stage_out(k):
        mate_copy(k).wait_recv()
        for which in range(2):
            rows = pl.ds((k * 2 + which) * step, step)
            mean = total[k, which].astype(jnp.float32) * (1.0 / member_count)
            out[:, rows] = (raw[:, rows].astype(jnp.float32) - mean).astype(jnp.bfloat16)

    stages = [stage_near, stage_sum]
    stages += [functools.partial(stage_line, level) for level in range(1, middle)]
    stages += [stage_swap]
    stages += [functools.partial(stage_back, level) for level in range(middle - 2, -1, -1)]
    stages += [stage_out]

    for k in range(parts):
        for hop in range(1, bands):
            spread(k, hop).start()
    raw[space] = sent[space]
    for turn in range(parts + len(stages) - 1):
        for place in reversed(range(len(stages))):
            k = turn - place
            if 0 <= k < parts:
                stages[place](k)

    for k in range(parts):
        for hop in range(1, bands):
            spread(k, hop).wait_send()
        near_copy(k).wait_send()
        mate_copy(k).wait_send()

        @pl.when(rank == middle - 1)
        def _():
            swap_copy(k).wait_send()

        @pl.when(rank < middle - 1)
        def _():
            line_copy(k).wait_send()

        @pl.when(rank > 0)
        def _():
            back_copy(k).wait_send()


def exchange(found):
    bands, depth, width = found.shape
    parts = next(p for p in (6, 3, 2, 1) if depth % (32 * p) == 0)
    step = depth // (2 * parts)
    buffer = pltpu.VMEM((parts, bands, step, width), jnp.bfloat16)
    dma = pltpu.SemaphoreType.DMA
    vmem = pl.BlockSpec(memory_space=pltpu.VMEM)
    return pl.pallas_call(
        functools.partial(exchange_kernel, parts),
        out_shape=jax.ShapeDtypeStruct(found.shape, jnp.bfloat16),
        in_specs=[vmem],
        out_specs=vmem,
        scratch_shapes=[
            pltpu.VMEM((bands, depth, width), jnp.bfloat16),
            buffer,
            buffer,
            buffer,
            buffer,
            pltpu.VMEM((parts, 2, bands, step, width), jnp.bfloat16),
            dma((parts, bands)),
            dma((parts, bands)),
        ]
        + [dma((parts,))] * 10,
        compiler_params=pltpu.CompilerParams(
            has_side_effects=True, vmem_limit_bytes=56 * 1024 * 1024
        ),
    )(found)


def local(weather, coefficients, channel_scale):
    group_count = lax.axis_size("member")
    band_count = lax.axis_size("space")
    member_local, channels, rows_local, lon_count = weather.shape
    order_local = coefficients.shape[3]
    degree_count = coefficients.shape[4]
    order_count = order_local * band_count
    lat_count = rows_local * band_count
    member_count = member_local * group_count
    rows = member_local * channels * 2
    half = round_up(order_local, 16) // 2
    padded = 2 * half
    degrees_padded = round_up(degree_count, 128)

    first_order = lax.axis_index("space") * order_local
    slots = jnp.arange(padded, dtype=jnp.int32)
    orders = first_order + slots
    logs = jnp.pad(diagonal_log(order_count), (0, padded))
    order_logs = lax.dynamic_slice_in_dim(logs, first_order, padded)
    row_first = (lon_count // 2 + 1 - lat_count) // 2
    colatitude = (
        math.pi
        * (row_first + jnp.arange(lat_count, dtype=jnp.int32)).astype(jnp.float32)
        / (lon_count // 2)
    )
    order_values = orders.astype(jnp.float32)[:, None]
    diagonal = jnp.exp(
        order_logs[:, None]
        - 0.5 * math.log(4.0 * math.pi)
        + order_values * jnp.log(jnp.sin(colatitude))[None, :]
    )

    def pair_up(plane):
        return jnp.concatenate([plane[:half], plane[half:]], axis=1)

    order_plane = pair_up(jnp.broadcast_to(order_values, (padded, lat_count)))
    cosine_row = jnp.tile(jnp.cos(colatitude), 2)[None, :]

    spectral = turn_spectral(
        coefficients.reshape(rows, order_local, degree_count), padded, degrees_padded, degree_count
    ).reshape(2, half, rows, degrees_padded)
    found = synthesize(spectral, order_plane, cosine_row, pair_up(diagonal), rows_local)
    depth = padded * 2
    flat = member_local * channels * rows_local
    found = found.reshape(band_count, depth, -1)
    centred = exchange(found)

    band = jnp.arange(band_count, dtype=jnp.int32)[:, None]
    slot = slots.reshape(2, half)
    row_order = band * order_local + slots[None, :]
    real_slot = jnp.broadcast_to(slots[None, :] < order_local, row_order.shape)
    columns = jnp.arange(lon_count, dtype=jnp.int32)
    phases = row_order[:, :, None] * columns % lon_count
    angles = 2.0 * math.pi / lon_count * phases.astype(jnp.float32)
    weights = jnp.where(real_slot, jnp.where(row_order == 0, 1.0, math.sqrt(2.0)), 0.0)
    weights = weights.astype(jnp.float32)[:, :, None]
    shape = (band_count, 2, half, lon_count)
    basis = jnp.stack(
        [(weights * jnp.cos(angles)).reshape(shape), (weights * jnp.sin(angles)).reshape(shape)], axis=2
    ).astype(jnp.bfloat16)
    basis = basis.reshape(band_count * depth, lon_count)

    centred = centred.reshape(band_count * depth, -1)[:, :flat]
    noise = lax.dot_general(
        centred, basis, (((0,), (0,)), ((), ())), preferred_element_type=jnp.float32
    )
    noise = noise.reshape(member_local, channels, rows_local, lon_count)
    scale_wide = channel_scale[None, :, None, None]
    return (weather.astype(jnp.float32) + scale_wide * noise).astype(jnp.bfloat16)


def solution(mesh):
    return jax.shard_map(
        local,
        mesh=mesh,
        in_specs=(P("member", None, "space", None), P("member", None, None, "space", None), P()),
        out_specs=P("member", None, "space", None),
        check_vma=False,
    )
```

```python
import functools
import math

import jax
import jax.numpy as jnp
from jax import lax
from jax.experimental import pallas as pl
from jax.experimental.pallas import tpu as pltpu
from jax.sharding import PartitionSpec as P


def round_up(value, step):
    return (value + step - 1) // step * step


def diagonal_log(order_count):
    steps_up = jnp.arange(1, order_count, dtype=jnp.int32).astype(jnp.float32)
    terms = 0.5 * jnp.log((2.0 * steps_up + 1.0) / (2.0 * steps_up))
    return jnp.concatenate([jnp.zeros((1,), jnp.float32), jnp.cumsum(terms)])


def synthesis_kernel(
    block, lat, order_ref, cosine_ref, diagonal_ref, coef, tail, out_ref, table, kept, held, arrived
):
    half, lanes = order_ref.shape
    channels, order_local, _, degree_count = coef.shape
    rows, tiles = held.shape[1], held.shape[2]
    degrees = tiles * 128
    pitch = degrees + 8
    factor = math.sqrt(3.0) * math.sqrt(4.0 * math.pi) / degree_count * 2.0 ** (-30)
    turn = pl.program_id(0)
    flat = held.reshape(held.shape[0] * rows * tiles * 2, 128)

    def fetch(step, act):
        base = lax.rem(step, 2) * (2 * block)
        for spot in range(2 * block):
            slot = step * block + spot % block + spot // block * half
            slot = jnp.minimum(slot, order_local - 1)
            for tile in range(tiles):
                if tile < tiles - 1:
                    source = coef.at[:, slot, :, pl.ds(tile * 128, 128)]
                else:
                    source = tail.at[:, slot]
                copy = pltpu.make_async_copy(
                    source,
                    held.at[base + spot, pl.ds(0, channels), tile],
                    arrived.at[base + spot, tile],
                )
                act(copy)

    @pl.when(turn == 0)
    def begin():
        fetch(turn, lambda copy: copy.start())

    @pl.when(turn + 1 < pl.num_programs(0))
    def ahead():
        fetch(turn + 1, lambda copy: copy.start())

    @pl.when(pl.program_id(0) == 0)
    def build():
        order = order_ref[...]
        order_square = order * order
        cosine = jnp.broadcast_to(cosine_ref[...], (half, lanes))
        diagonal = diagonal_ref[...]

        def advance(step, carry):
            older, newer, down = carry
            degree = step.astype(jnp.float32)
            wide = jnp.full((half, lanes), degree, jnp.float32)
            square = wide * wide
            ratio = jnp.maximum(square - order_square, 0.25) / jnp.maximum(4.0 * square - 1.0, 1.0)
            up = lax.rsqrt(ratio)
            row = up * (cosine * newer - down * older)
            row = jnp.where(wide < order, 0.0, jnp.where(wide == order, diagonal, row))
            for tile in range(lanes // 128):
                table[pl.ds(tile * half * pitch + step, half, stride=pitch), :] = row[
                    :, tile * 128 : tile * 128 + 128
                ]
            return newer, row, ratio * up

        zero = order * 0.0
        lax.fori_loop(0, degrees, advance, (zero, zero, zero), unroll=4)

    fetch(turn, lambda copy: copy.wait())
    first = turn * block
    low = lax.broadcasted_iota(jnp.int32, (rows, lanes), 1) < lanes // 2
    pack = 128 // lat
    bands = lanes // 2 // lat
    groups = out_ref.shape[-1] // 128
    deep = half + 8
    lane = lax.broadcasted_iota(jnp.int32, (rows, 128), 1)
    first_order = lax.axis_index("space") * order_local

    def read(spot, slot, part):
        base = (lax.rem(turn, 2) * (2 * block) + spot) * (rows * tiles * 2)
        pieces = []
        for tile in range(tiles):
            values = flat[pl.ds(base + tile * 2 + part, rows, stride=tiles * 2), :]
            degree = lane + tile * 128
            least = jnp.where(slot < order_local, first_order + slot, degrees)
            keep = (degree >= least) & (degree < degree_count)
            pieces.append(jnp.where(keep, values.astype(jnp.float32) * factor, 0.0))
        return jnp.concatenate(pieces, axis=1)

    for inner in range(block):
        columns = []
        for tile in range(lanes // 128):
            start = pl.multiple_of((tile * half + first + inner) * pitch, 8)
            columns.append(table[pl.ds(start, degrees), :].astype(jnp.bfloat16))
        values = jnp.concatenate(columns, axis=1)
        stacked = [
            read(inner + side * block, first + inner + side * half, part)
            for side in range(2)
            for part in range(2)
        ]
        stacked = jnp.concatenate(stacked, axis=0).astype(jnp.bfloat16)
        found = jnp.dot(stacked, values, preferred_element_type=jnp.float32)
        for part in range(2):
            one = found[part * rows : part * rows + rows]
            two = found[(2 + part) * rows : (3 + part) * rows]
            merged = jnp.where(low, one, two)
            for tile in range(lanes // 128):
                start = (tile * 2 + part) * rows * deep + first + inner
                kept[pl.ds(start, rows, stride=deep), :] = merged[:, tile * 128 : tile * 128 + 128]

    @pl.when(pl.program_id(0) == pl.num_programs(0) - 1)
    def regroup():
        chunk = lax.broadcasted_iota(jnp.int32, (half, 128), 1) // lat
        for tile in range(lanes // 128):
            def one_group(group, carry):
                for part in range(2):
                    planes = []
                    for spot in range(pack):
                        row = (tile * 2 + part) * rows + group * pack + spot
                        planes.append(kept[pl.ds(pl.multiple_of(row * deep, 8), half), :])
                    gap = 1
                    while gap < pack:
                        upper = (chunk // gap) % 2 == 1
                        for spot in range(pack):
                            if (spot // gap) % 2 == 0:
                                one, two = planes[spot], planes[spot + gap]
                                planes[spot] = jnp.where(upper, pltpu.roll(two, gap * lat, 1), one)
                                planes[spot + gap] = jnp.where(
                                    upper, two, pltpu.roll(one, 128 - gap * lat, 1)
                                )
                        gap *= 2
                    for spot in range(pack):
                        high, band = divmod(tile * pack + spot, bands)
                        lane = pl.multiple_of(group * 128, 128)
                        out_ref[band, high, part, :, pl.ds(lane, 128)] = planes[spot].astype(
                            jnp.bfloat16
                        )
                return carry

            lax.fori_loop(0, groups, one_group, 0)


def synthesize(coefficients, order_plane, cosine_row, diagonal_plane, lat):
    channels, _, _, degree_count = coefficients.shape
    half, lanes = order_plane.shape
    block = 8
    tiles = round_up(degree_count, 128) // 128
    rows = round_up(channels, 8)
    tail = coefficients[..., (tiles - 1) * 128 :]
    tail = jnp.pad(tail, ((0, 0), (0, 0), (0, 0), (0, tiles * 128 - degree_count)))
    groups = round_up(channels, 128 // lat) // (128 // lat)
    out_dims = (lanes // 2 // lat, 2, 2, half, groups * 128)
    return pl.pallas_call(
        functools.partial(synthesis_kernel, block, lat),
        grid=(half // block,),
        out_shape=jax.ShapeDtypeStruct(out_dims, jnp.bfloat16),
        in_specs=[
            pl.BlockSpec((half, lanes), lambda i: (0, 0)),
            pl.BlockSpec((1, lanes), lambda i: (0, 0)),
            pl.BlockSpec((half, lanes), lambda i: (0, 0)),
            pl.BlockSpec(memory_space=pl.ANY),
            pl.BlockSpec(memory_space=pl.ANY),
        ],
        out_specs=pl.BlockSpec(out_dims, lambda i: (0, 0, 0, 0, 0)),
        scratch_shapes=[
            pltpu.VMEM((lanes // 128 * half * (tiles * 128 + 8), 128), jnp.float32),
            pltpu.VMEM((lanes // 128 * 2 * rows * (half + 8), 128), jnp.float32),
            pltpu.VMEM((4 * block, rows, tiles, 2, 128), jnp.int32),
            pltpu.SemaphoreType.DMA((4 * block, tiles)),
        ],
        compiler_params=pltpu.CompilerParams(vmem_limit_bytes=60 * 1024 * 1024),
    )(order_plane, cosine_row, diagonal_plane, coefficients, tail)


def exchange_kernel(parts, sent, out, raw, near, sums, lower, other, total, *sems):
    a2a_send, a2a_recv = sems[0], sems[1]
    pair = {
        "near": (sems[2], sems[3]),
        "line": (sems[4], sems[5]),
        "swap": (sems[6], sems[7]),
        "back": (sems[8], sems[9]),
        "mate": (sems[10], sems[11]),
    }
    bands, depth, _ = sent.shape
    member_count = lax.axis_size("member")
    chips = member_count // 2
    middle = chips // 2
    me = lax.axis_index("member")
    space = lax.axis_index("space")
    core = lax.rem(me, 2)
    chip = me // 2
    mate = chip * 2 + 1 - core
    left = chip < middle
    rank = jnp.where(left, chip, chips - 1 - chip)
    inward = jnp.where(left, chip + 1, chip - 1) * 2 + core
    outward = jnp.where(left, chip - 1, chip + 1) * 2 + core
    step = depth // (2 * parts)
    mesh_ids = pl.DeviceIdType.MESH

    def spread(k, hop):
        rows = pl.ds(k * 2 * step, 2 * step)
        target = lax.rem(space + hop, bands)
        return pltpu.make_async_remote_copy(
            src_ref=sent.at[target, rows],
            dst_ref=raw.at[space, rows],
            send_sem=a2a_send.at[k, hop],
            recv_sem=a2a_recv.at[k, hop],
            device_id={"space": target},
            device_id_type=mesh_ids,
        )

    def hand(kind, k, source, landing, target):
        return pltpu.make_async_remote_copy(
            src_ref=source,
            dst_ref=landing,
            send_sem=pair[kind][0].at[k],
            recv_sem=pair[kind][1].at[k],
            device_id={"member": target},
            device_id_type=mesh_ids,
        )

    def half_rows(k, which):
        return pl.ds(pl.multiple_of((k * 2 + which) * step, step), step)

    def near_copy(k):
        return hand("near", k, raw.at[:, half_rows(k, 1 - core)], near.at[k], mate)

    def line_copy(k):
        return hand("line", k, sums.at[k], lower.at[k], inward)

    def swap_copy(k):
        return hand("swap", k, sums.at[k], other.at[k], inward)

    def back_copy(k):
        return hand("back", k, total.at[k, core], total.at[k, core], outward)

    def mate_copy(k):
        return hand("mate", k, total.at[k, core], total.at[k, core], mate)

    def stage_near(k):
        for hop in range(1, bands):
            spread(k, hop).wait_recv()
        near_copy(k).start()

    def send_inward(k, level):
        @pl.when(rank == level)
        def _():
            if level == middle - 1:
                swap_copy(k).start()
            else:
                line_copy(k).start()

    def stage_sum(k):
        near_copy(k).wait_recv()
        mine = raw[:, half_rows(k, core)].astype(jnp.float32) + near[k].astype(jnp.float32)
        sums[k] = mine.astype(jnp.bfloat16)
        send_inward(k, 0)

    def stage_line(level, k):
        @pl.when(rank == level)
        def _():
            line_copy(k).wait_recv()
            both = sums[k].astype(jnp.float32) + lower[k].astype(jnp.float32)
            sums[k] = both.astype(jnp.bfloat16)

        send_inward(k, level)

    def send_outward(k, level):
        if level > 0:
            back_copy(k).start()
        mate_copy(k).start()

    def stage_swap(k):
        @pl.when(rank == middle - 1)
        def _():
            swap_copy(k).wait_recv()
            both = sums[k].astype(jnp.float32) + other[k].astype(jnp.float32)
            total[k, core] = both.astype(jnp.bfloat16)
            send_outward(k, middle - 1)

    def stage_back(level, k):
        @pl.when(rank == level)
        def _():
            back_copy(k).wait_recv()
            send_outward(k, level)

    def stage_out(k):
        mate_copy(k).wait_recv()
        for which in range(2):
            rows = pl.ds((k * 2 + which) * step, step)
            mean = total[k, which].astype(jnp.float32) * (1.0 / member_count)
            out[:, rows] = (raw[:, rows].astype(jnp.float32) - mean).astype(jnp.bfloat16)

    stages = [stage_near, stage_sum]
    stages += [functools.partial(stage_line, level) for level in range(1, middle)]
    stages += [stage_swap]
    stages += [functools.partial(stage_back, level) for level in range(middle - 2, -1, -1)]
    stages += [stage_out]

    for k in range(parts):
        for hop in range(1, bands):
            spread(k, hop).start()
    raw[space] = sent[space]
    for turn in range(parts + len(stages) - 1):
        for place in reversed(range(len(stages))):
            k = turn - place
            if 0 <= k < parts:
                stages[place](k)

    for k in range(parts):
        for hop in range(1, bands):
            spread(k, hop).wait_send()
        near_copy(k).wait_send()
        mate_copy(k).wait_send()

        @pl.when(rank == middle - 1)
        def _():
            swap_copy(k).wait_send()

        @pl.when(rank < middle - 1)
        def _():
            line_copy(k).wait_send()

        @pl.when(rank > 0)
        def _():
            back_copy(k).wait_send()


def exchange(found):
    bands, depth, width = found.shape
    parts = next(p for p in (6, 3, 2, 1) if depth % (32 * p) == 0)
    step = depth // (2 * parts)
    buffer = pltpu.VMEM((parts, bands, step, width), jnp.bfloat16)
    dma = pltpu.SemaphoreType.DMA
    vmem = pl.BlockSpec(memory_space=pltpu.VMEM)
    return pl.pallas_call(
        functools.partial(exchange_kernel, parts),
        out_shape=jax.ShapeDtypeStruct(found.shape, jnp.bfloat16),
        in_specs=[vmem],
        out_specs=vmem,
        scratch_shapes=[
            pltpu.VMEM((bands, depth, width), jnp.bfloat16),
            buffer,
            buffer,
            buffer,
            buffer,
            pltpu.VMEM((parts, 2, bands, step, width), jnp.bfloat16),
            dma((parts, bands)),
            dma((parts, bands)),
        ]
        + [dma((parts,))] * 10,
        compiler_params=pltpu.CompilerParams(
            has_side_effects=True, vmem_limit_bytes=56 * 1024 * 1024
        ),
    )(found)


def basis_kernel(fine_cos, fine_sin, coarse_cos, coarse_sin, out):
    lon_count = out.shape[-1]
    for high in range(2):
        cos_b, sin_b = fine_cos[0, high], fine_sin[0, high]
        for start in range(0, lon_count, 128):
            tile = start // 128
            width = min(128, lon_count - start)
            cos_a = coarse_cos[0, high, :, tile : tile + 1]
            sin_a = coarse_sin[0, high, :, tile : tile + 1]
            real = (cos_a * cos_b - sin_a * sin_b).astype(jnp.bfloat16)
            imag = (sin_a * cos_b + cos_a * sin_b).astype(jnp.bfloat16)
            out[0, high, 0, :, start : start + width] = real[:, :width]
            out[0, high, 1, :, start : start + width] = imag[:, :width]


def make_basis(fine_cos, fine_sin, coarse_cos, coarse_sin, lon_count):
    bands, _, half, lanes = fine_cos.shape
    spec = pl.BlockSpec((1, 2, half, lanes), lambda i: (i, 0, 0, 0))
    return pl.pallas_call(
        basis_kernel,
        grid=(bands,),
        out_shape=jax.ShapeDtypeStruct((bands, 2, 2, half, lon_count), jnp.bfloat16),
        in_specs=[spec] * 4,
        out_specs=pl.BlockSpec((1, 2, 2, half, lon_count), lambda i: (i, 0, 0, 0, 0)),
    )(fine_cos, fine_sin, coarse_cos, coarse_sin)


def local(weather, coefficients, channel_scale):
    group_count = lax.axis_size("member")
    band_count = lax.axis_size("space")
    member_local, channels, rows_local, lon_count = weather.shape
    order_local = coefficients.shape[3]
    degree_count = coefficients.shape[4]
    order_count = order_local * band_count
    lat_count = rows_local * band_count
    member_count = member_local * group_count
    half = round_up(order_local, 16) // 2
    padded = 2 * half

    first_order = lax.axis_index("space") * order_local
    slots = jnp.arange(padded, dtype=jnp.int32)
    orders = first_order + slots
    logs = jnp.pad(diagonal_log(order_count), (0, padded))
    order_logs = lax.dynamic_slice_in_dim(logs, first_order, padded)
    row_first = (lon_count // 2 + 1 - lat_count) // 2
    colatitude = (
        math.pi
        * (row_first + jnp.arange(lat_count, dtype=jnp.int32)).astype(jnp.float32)
        / (lon_count // 2)
    )
    order_values = orders.astype(jnp.float32)[:, None]
    diagonal = jnp.exp(
        order_logs[:, None]
        - 0.5 * math.log(4.0 * math.pi)
        + order_values * jnp.log(jnp.sin(colatitude))[None, :]
    )

    def pair_up(plane):
        return jnp.concatenate([plane[:half], plane[half:]], axis=1)

    order_plane = pair_up(jnp.broadcast_to(order_values, (padded, lat_count)))
    cosine_row = jnp.tile(jnp.cos(colatitude), 2)[None, :]

    turned = coefficients.transpose(0, 1, 3, 2, 4)
    turned = turned.reshape(member_local * channels, order_local, 2, degree_count)
    found = synthesize(turned, order_plane, cosine_row, pair_up(diagonal), rows_local)
    depth = padded * 2
    flat = member_local * channels * rows_local
    found = found.reshape(band_count, depth, -1)
    centred = exchange(found)

    band = jnp.arange(band_count, dtype=jnp.int32)[:, None]
    slot = slots.reshape(2, half)
    row_order = band * order_local + slots[None, :]
    real_slot = jnp.broadcast_to(slots[None, :] < order_local, row_order.shape)
    weights = jnp.where(real_slot, jnp.where(row_order == 0, 1.0, math.sqrt(2.0)), 0.0)
    weights = weights.astype(jnp.float32)[:, :, None]

    def waves(steps):
        phases = row_order[:, :, None] * steps % lon_count
        angles = 2.0 * math.pi / lon_count * phases.astype(jnp.float32)
        shape = (band_count, 2, half, 128)
        return jnp.cos(angles).reshape(shape), jnp.sin(angles).reshape(shape)

    lanes = jnp.arange(128, dtype=jnp.int32)
    fine = waves(lanes)
    heavy = jnp.broadcast_to(weights, (band_count, padded, 128)).reshape(band_count, 2, half, 128)
    coarse = [heavy * wave for wave in waves(lanes * 128 % lon_count)]
    basis = make_basis(*fine, *coarse, lon_count).reshape(band_count * depth, lon_count)

    centred = centred.reshape(band_count * depth, -1)[:, :flat]
    noise = lax.dot_general(
        centred, basis, (((0,), (0,)), ((), ())), preferred_element_type=jnp.float32
    )
    noise = noise.reshape(member_local, channels, rows_local, lon_count)
    scale_wide = channel_scale[None, :, None, None]
    return (weather.astype(jnp.float32) + scale_wide * noise).astype(jnp.bfloat16)


def solution(mesh):
    return jax.shard_map(
        local,
        mesh=mesh,
        in_specs=(P("member", None, "space", None), P("member", None, None, "space", None), P()),
        out_specs=P("member", None, "space", None),
        check_vma=False,
    )
```
